32 devices in a mesh: row: 4 (over z), col: 8 (over y, x, core).
Axes of the slice: x: 2, y: 2, z: 4, core: 2. Of those that a mesh axis runs over, the one named last changes fastest.
Arguments:
- query_grid: bfloat16 [64, 64, 6144], P('row', 'col'), may hold values from -6 to 6
- key_grid: bfloat16 [64, 64, 6144], P('row', 'col'), may hold values from -6 to 6
- value_grid: bfloat16 [64, 64, 6144], P('row', 'col'), may hold values from -6 to 6
- sink_keys: bfloat16 [8, 6144], replicated, may hold values from -9 to 9
- sink_values: bfloat16 [8, 6144], replicated, may hold values from -6 to 6
- grad_output: bfloat16 [64, 64, 6144], P('row', 'col'), may hold values from -6 to 6
- block_input: bfloat16 [64, 64, 6144], P('row', 'col'), may hold values from -6 to 6
- in_weight: bfloat16 [6144, 12288], P(None, 'col'), may hold values from -0.078125 to 0.078125
- in_bias: float32 [12288], P('col'), may hold values from -3 to 3
Outputs:
- attn_out: bfloat16 [64, 64, 6144], P('row', 'col')
- grad_query: bfloat16 [64, 64, 6144], P('row', 'col')
- grad_key: bfloat16 [64, 64, 6144], P('row', 'col')
- grad_value: bfloat16 [64, 64, 6144], P('row', 'col')
- grad_sink_keys: bfloat16 [8, 6144], replicated
- grad_sink_values: bfloat16 [8, 6144], replicated
- hidden: bfloat16 [64, 64, 12288], P('row', None, 'col')
The draws below stay inside these ranges and needn't reach their ends.
All inputs are finite; a program needn't handle non-finite values.
Results may differ from the reference program's by a relative error of at most 0.017.
Values may be sent and summed in bfloat16 or wider, within the bound.
A program may use at most 192 MiB of HBM per device.

```python
import math
import jax
import jax.numpy as jnp
from jax import lax

D = 6144
HEADS = 48
HEAD_DIM = 128
FF_W = 12288
WIN = 16
REGS = 8
GRID_R = 64
GRID_C = 64


def paired_fields(key):
    key_q, key_k = jax.random.split(key, 2)
    shape = (GRID_R, GRID_C, D)
    query = jnp.clip(jax.random.normal(key_q, shape, jnp.float32), -6.0, 6.0)
    keyed = jnp.clip(jax.random.normal(key_k, shape, jnp.float32), -6.0, 6.0)
    return (query, keyed)


def draw_query_grid(key, part):
    return paired_fields(jax.random.fold_in(key, 11))[0].astype(jnp.bfloat16)


def draw_key_grid(key, part):
    return paired_fields(jax.random.fold_in(key, 11))[1].astype(jnp.bfloat16)


def levels(key, dims, shards, least, high):
    def one(position, parts):
        steps = jax.random.uniform(jax.random.fold_in(jax.random.fold_in(key, 6), position), (parts,), jnp.float32, least / len(shards), high / len(shards))
        return jnp.repeat(jnp.exp(steps), dims[position] // parts).reshape((-1,) + (1,) * (len(dims) - position - 1))

    level = one(*shards[0])
    for cut in shards[1:]:
        level = level * one(*cut)
    return level


def noise(stream_key, shape, scale, limit, cuts=(), kind=jnp.bfloat16):
    array = scale * jax.random.normal(stream_key, shape, jnp.float32)
    if cuts:
        array = array * levels(stream_key, shape, cuts, -0.22, 0.18)
    return jnp.clip(array, -limit, limit).astype(kind)


def setup_inputs(seed: int = 0) -> dict:
    key_of = jax.random.split(jax.random.key(seed), 10)
    query_grid = draw_query_grid(jax.random.fold_in(key_of[9], 71), 0)
    key_grid = draw_key_grid(jax.random.fold_in(key_of[9], 71), 0)
    value_grid = noise(key_of[2], (GRID_R, GRID_C, D), 1.0, 6.0, ((0, 4), (1, 8)))
    sink_keys = noise(key_of[3], (REGS, D), 1.5, 9.0)
    sink_values = noise(key_of[4], (REGS, D), 1.0, 6.0)
    grad_output = noise(key_of[5], (GRID_R, GRID_C, D), 1.0, 6.0, ((0, 4), (1, 8)))
    block_input = noise(key_of[6], (GRID_R, GRID_C, D), 1.0, 6.0, ((0, 4), (1, 8)))
    in_weight = noise(key_of[7], (D, FF_W), D ** -0.5, 0.078125, ((1, 8),))
    in_bias = noise(key_of[8], (FF_W,), 0.5, 3.0, ((0, 8),), jnp.float32)
    return dict(query_grid=query_grid, key_grid=key_grid, value_grid=value_grid, sink_keys=sink_keys, sink_values=sink_values, grad_output=grad_output, block_input=block_input, in_weight=in_weight, in_bias=in_bias)


def product(form, left, right):
    return jnp.einsum(form, left.astype(jnp.float32), right.astype(jnp.float32))

def attend(query, key_rows, value_rows, sink_k, sink_v, grad_out):
    score_scale = 1.0 / math.sqrt(query.shape[-1])
    window_scores = product('qhe,khe->hqk', query, key_rows) * score_scale
    sink_scores = product('qhe,rhe->hqr', query, sink_k) * score_scale
    row_max = jnp.maximum(lax.optimization_barrier(jnp.max(window_scores, axis=-1, keepdims=True)), lax.optimization_barrier(jnp.max(sink_scores, axis=-1, keepdims=True)))
    window_exp = jnp.exp(window_scores - row_max)
    sink_exp = jnp.exp(sink_scores - row_max)
    row_total = lax.optimization_barrier(jnp.sum(window_exp, axis=-1, keepdims=True)) + lax.optimization_barrier(jnp.sum(sink_exp, axis=-1, keepdims=True))
    window_prob = window_exp / row_total
    sink_prob = sink_exp / row_total
    window_weight = window_prob.astype(jnp.bfloat16)
    sink_weight = sink_prob.astype(jnp.bfloat16)
    mixed = product('hqk,khe->qhe', window_weight, value_rows) + product('hqr,rhe->qhe', sink_weight, sink_v)
    attended = mixed.astype(jnp.bfloat16)
    row_delta = lax.optimization_barrier(jnp.sum(grad_out.astype(jnp.float32) * attended.astype(jnp.float32), axis=-1)).T[:, :, None]
    window_dprob = product('qhe,khe->hqk', grad_out, value_rows)
    sink_dprob = product('qhe,rhe->hqr', grad_out, sink_v)
    window_dscore = (window_prob * (window_dprob - row_delta) * score_scale).astype(jnp.bfloat16)
    sink_dscore = (sink_prob * (sink_dprob - row_delta) * score_scale).astype(jnp.bfloat16)
    grad_q = (product('hqk,khe->qhe', window_dscore, key_rows) + product('hqr,rhe->qhe', sink_dscore, sink_k)).astype(jnp.bfloat16)
    grad_k = product('hqk,qhe->khe', window_dscore, query)
    grad_v = product('hqk,qhe->khe', window_weight, grad_out)
    sink_gk = product('hqr,qhe->rhe', sink_dscore, query)
    sink_gv = product('hqr,qhe->rhe', sink_weight, grad_out)
    return (attended, grad_q, grad_k, grad_v, sink_gk, sink_gv)

def to_windows(grid):
    blocks = grid.reshape(GRID_R // WIN, WIN, GRID_C // WIN, WIN, HEADS, HEAD_DIM)
    return blocks.transpose(0, 2, 1, 3, 4, 5).reshape(-1, WIN * WIN, HEADS, HEAD_DIM)

def from_windows(blocks):
    grid = blocks.reshape(GRID_R // WIN, GRID_C // WIN, WIN, WIN, HEADS * HEAD_DIM)
    return grid.transpose(0, 2, 1, 3, 4).reshape(GRID_R, GRID_C, HEADS * HEAD_DIM)

def reference(query_grid, key_grid, value_grid, sink_keys, sink_values, grad_output, block_input, in_weight, in_bias):
    sink_k = sink_keys.reshape(REGS, HEADS, HEAD_DIM)
    sink_v = sink_values.reshape(REGS, HEADS, HEAD_DIM)

    def advance(carry, blocks):
        results = attend(blocks[0], blocks[1], blocks[2], sink_k, sink_v, blocks[3])
        carry = (carry[0] + results[4], carry[1] + results[5])
        return (carry, (results[0], results[1], results[2].astype(jnp.bfloat16), results[3].astype(jnp.bfloat16)))
    start = jnp.zeros((REGS, HEADS, HEAD_DIM), jnp.float32)
    inputs = (to_windows(query_grid), to_windows(key_grid), to_windows(value_grid), to_windows(grad_output))
    sums, outputs = lax.scan(advance, (start, start), inputs)
    attn_out = from_windows(outputs[0])
    grad_query = from_windows(outputs[1])
    grad_key = from_windows(outputs[2])
    grad_value = from_windows(outputs[3])
    grad_sink_keys = sums[0].reshape(REGS, HEADS * HEAD_DIM).astype(jnp.bfloat16)
    grad_sink_values = sums[1].reshape(REGS, HEADS * HEAD_DIM).astype(jnp.bfloat16)
    projected = jnp.dot(block_input, in_weight, preferred_element_type=jnp.float32) + in_bias
    hidden = jax.nn.gelu(projected, approximate=False).astype(jnp.bfloat16)
    return (attn_out, grad_query, grad_key, grad_value, grad_sink_keys, grad_sink_values, hidden)
```

```python
import functools
import math

import jax
import jax.numpy as jnp
from jax import lax
from jax.experimental import pallas as pl
from jax.experimental.pallas import tpu as pltpu
from jax.sharding import PartitionSpec as P

HEAD_DIM = 128
WIN = 16
MESH = pl.DeviceIdType.MESH
F32 = jnp.float32
BF16 = jnp.bfloat16
CHUNKS = 12
GROUPS = 8
UNROLL = 2
NT = 512
PIECES = 6
WPARTS = 6
VMEM_LIMIT = 50 * 1024 * 1024


def bits(r):
    return bin(r).count("1")


def parent(r, tree):
    if tree == 0:
        return r & ~(1 << (r.bit_length() - 1))
    return r & (r - 1)


def dot_nt(a, b):
    return lax.dot_general(a, b, (((1,), (1,)), ((), ())), preferred_element_type=F32)


def dot_nn(a, b):
    return lax.dot_general(a, b, (((1,), (0,)), ((), ())), preferred_element_type=F32)


def dot_tn(a, b):
    return lax.dot_general(a, b, (((0,), (0,)), ((), ())), preferred_element_type=F32)


def kernel(
    rows,
    cols,
    q_in,
    k_in,
    v_in,
    g_in,
    x_in,
    w_in,
    sk_in,
    sv_in,
    bias,
    gb,
    qb,
    kb,
    vb,
    fin,
    hid,
    pk,
    pv,
    rk,
    rv,
    xg,
    wv,
    acc,
    sg,
    ra,
    sb,
    rb,
    rc,
    sk,
    sv,
    load_sem,
    w_sem,
    xs_sem,
    xr_sem,
    ps_sem,
    pr_sem,
    kvs_sem,
    kvr_sem,
    gs_sem,
    gr_sem,
    a_sem,
    b_send,
    b_recv,
    c_send,
    c_recv,
    d_send,
    d_recv,
    e_sem,
):
    tokens, width = q_in.shape
    units = w_in.shape[1]
    regs = fin.shape[1]
    chips = cols // 2
    levels = chips.bit_length() - 1
    last = chips - 1
    heads = width // HEAD_DIM
    per_group = heads // GROUPS
    kc = width // CHUNKS
    gw = width // GROUPS
    rw = width // rows
    wk = width // WPARTS
    pw = width // PIECES
    pair = 2 * tokens
    scale = 1.0 / math.sqrt(HEAD_DIM)
    nt = min(NT, units)
    n_tiles = units // nt

    my_row = lax.axis_index("row")
    my_col = lax.axis_index("col")
    parity = my_col % 2
    chip = my_col // 2
    peer = (my_row, my_col + 1 - 2 * parity)

    def flipped(value, mask):
        for b in range(levels):
            if mask >> b & 1:
                value = value + (1 << b) * (1 - 2 * ((value // (1 << b)) % 2))
        return value

    def chip_dev(r):
        return (my_row, flipped(chip, r) * 2 + parity)

    def row_dev(d):
        return ((my_row + d) % rows, my_col)

    def kids(r, tree):
        return [k for k in range(1, chips) if parent(k, tree) == r]

    def load(src, dst, s):
        return pltpu.make_async_copy(src, dst, load_sem.at[s])

    own_rows = pl.ds(pl.multiple_of(my_col * tokens, tokens), tokens)
    grads = ((q_in, qb), (k_in, kb), (v_in, vb), (g_in, gb))
    load(x_in, xg.at[own_rows, :], 4).start()
    for s, (src, dst) in enumerate(grads):
        load(src, dst, s).start()

    barrier = pltpu.get_barrier_semaphore()
    pl.semaphore_signal(barrier, inc=1, device_id=peer, device_id_type=MESH)
    for r in range(1, chips):
        pl.semaphore_signal(barrier, inc=1, device_id=chip_dev(r), device_id_type=MESH)
    for d in range(1, rows):
        pl.semaphore_signal(barrier, inc=1, device_id=row_dev(d), device_id_type=MESH)

    for pad, given in ((sk, sk_in), (sv, sv_in)):
        pad[...] = jnp.zeros_like(pad)
        pad[:regs, :] = given[...]

    pl.semaphore_wait(barrier, 1 + chips - 1 + rows - 1)

    def group_cols(t):
        return pl.ds(pl.multiple_of(t * gw, gw), gw)

    def kv_copy(t, which):
        src, dst = ((k_in, pk), (v_in, pv))[which]
        c = group_cols(t)
        return pltpu.make_async_remote_copy(
            src_ref=src.at[:, c],
            dst_ref=dst.at[:, c],
            send_sem=kvs_sem.at[t, which],
            recv_sem=kvr_sem.at[t, which],
            device_id=peer,
            device_id_type=MESH,
        )

    def grad_copy(t, which):
        src, dst = ((pk, rk), (pv, rv))[which]
        c = group_cols(t)
        return pltpu.make_async_remote_copy(
            src_ref=src.at[:, c],
            dst_ref=dst.at[:, c],
            send_sem=gs_sem.at[t, which],
            recv_sem=gr_sem.at[t, which],
            device_id=peer,
            device_id_type=MESH,
        )

    def piece(c, r, core):
        origin = flipped(chip, r) * 2 + core
        return xg.at[
            pl.ds(pl.multiple_of(origin * tokens, tokens), tokens),
            pl.ds(pl.multiple_of(c * kc, kc), kc),
        ]

    def hop(c, r, up):
        block = piece(c, up, parity)
        return pltpu.make_async_remote_copy(
            src_ref=block,
            dst_ref=block,
            send_sem=xs_sem.at[c, r],
            recv_sem=xr_sem.at[c, r],
            device_id=chip_dev(up ^ r),
            device_id_type=MESH,
        )

    def hop_in(c, r):
        block = piece(c, r, parity)
        return pltpu.make_async_remote_copy(
            src_ref=block,
            dst_ref=block,
            send_sem=xs_sem.at[c, r],
            recv_sem=xr_sem.at[c, r],
            device_id=chip_dev(1),
            device_id_type=MESH,
        )

    def share(c, r):
        block = piece(c, r, parity)
        return pltpu.make_async_remote_copy(
            src_ref=block,
            dst_ref=block,
            send_sem=ps_sem.at[c, r],
            recv_sem=pr_sem.at[c, r],
            device_id=peer,
            device_id_type=MESH,
        )

    def share_in(c, r):
        block = piece(c, r, 1 - parity)
        return pltpu.make_async_remote_copy(
            src_ref=block,
            dst_ref=block,
            send_sem=ps_sem.at[c, r],
            recv_sem=pr_sem.at[c, r],
            device_id=peer,
            device_id_type=MESH,
        )

    def w_copy(c):
        part = pl.ds(pl.multiple_of(c * wk, wk), wk)
        return pltpu.make_async_copy(w_in.at[part, :], wv.at[part, :], w_sem.at[c])

    firsts = [r for r in range(1, chips) if bits(r) == 1]

    def pass_on(j, r, tree):
        c = 2 * j + tree
        hop_in(c, r).wait_recv()
        for kid in kids(r, tree):
            hop(c, kid, r).start()
        share(c, r).start()

    def forward(j):
        for r in firsts:
            for tree in range(2):
                if kids(r, tree):
                    pass_on(j, r, tree)

    def settle(j):
        for r in firsts:
            for tree in range(2):
                if not kids(r, tree):
                    pass_on(j, r, tree)

    half = CHUNKS // 2

    for which in range(2):
        kv_copy(0, which).start()
    load(x_in, xg.at[own_rows, :], 4).wait()
    for leaf in range(2):

        @pl.loop(0, half)
        def _(j):
            for r in firsts:
                for tree in range(2):
                    if bool(kids(r, tree)) != bool(leaf):
                        hop(2 * j + tree, r, 0).start()

    @pl.loop(1, GROUPS)
    def _(t):
        for which in range(2):
            kv_copy(t, which).start()

    @pl.loop(0, CHUNKS)
    def _(c):
        share(c, 0).start()

    @pl.loop(0, WPARTS)
    def _(c):
        w_copy(c).start()

    for s, (src, dst) in enumerate(grads):
        load(src, dst, s).wait()

    lane = lax.broadcasted_iota(jnp.int32, (tokens, HEAD_DIM), 1)

    def attend(first):
        at = [
            pl.ds(pl.multiple_of((first + j) * HEAD_DIM, HEAD_DIM), HEAD_DIM)
            for j in range(UNROLL)
        ]
        blank = jnp.zeros((HEAD_DIM - sk.shape[0], HEAD_DIM), BF16)
        done = []
        for c in at:
            q = qb[:, c]
            g = gb[:, c]
            keys = jnp.concatenate([kb[:, c], pk[:, c], sk[:, c], blank], axis=0)
            values = jnp.concatenate([vb[:, c], pv[:, c], sv[:, c], blank], axis=0)
            s = dot_nt(q, keys) * scale
            sw = s[:, : 2 * tokens]
            ss = jnp.where(lane < regs, s[:, 2 * tokens :], -1e30)
            s = jnp.concatenate([sw, ss], axis=1)
            e = jnp.exp(s - jnp.max(s, axis=-1, keepdims=True))
            p = e * (1.0 / jnp.sum(e, axis=-1, keepdims=True))
            weight = p.astype(BF16)
            o = dot_nn(weight, values).astype(BF16)
            delta = jnp.sum(g.astype(F32) * o.astype(F32), axis=-1, keepdims=True)
            dp = dot_nt(g, values)
            ds = (p * (dp - delta) * scale).astype(BF16)
            dq = dot_nn(ds, keys).astype(BF16)
            dk = dot_tn(ds, q)
            dv = dot_tn(weight, g)
            done.append((o, dq, dk, dv))
        for c, (o, dq, dk, dv) in zip(at, done):
            gb[:, c] = o
            qb[:, c] = dq
            kb[:, c] = dk[:tokens].astype(BF16)
            pk[:, c] = dk[tokens : 2 * tokens].astype(BF16)
            vb[:, c] = dv[:tokens].astype(BF16)
            pv[:, c] = dv[tokens : 2 * tokens].astype(BF16)
            sg[0, :, c] = dk[2 * tokens : 2 * tokens + regs]
            sg[1, :, c] = dv[2 * tokens : 2 * tokens + regs]

    def rows_of(r):
        return pl.ds(pl.multiple_of(flipped(chip, r) * pair, pair), pair)

    def finish(z, r, ncols):
        y = 0.5 * z * (1.0 + lax.erf(z * math.sqrt(0.5)))
        y = y.astype(BF16)
        per = tokens // WIN
        first = flipped(chip, r) * (2 * per)
        for j in range(2):
            hid[:, pl.ds(pl.multiple_of(first + j * per, per), per), ncols] = y[
                j * tokens : (j + 1) * tokens
            ].reshape(WIN, per, nt)

    def tile_cols(n):
        return pl.ds(pl.multiple_of(n * nt, nt), nt)

    def whole_rows(r, n):
        ncols = tile_cols(n)
        z = dot_nn(xg[rows_of(r), :], wv[:, ncols]) + bias[ncols]
        finish(z, r, ncols)

    def a_copy():
        return pltpu.make_async_remote_copy(
            src_ref=sg.at[1 - parity],
            dst_ref=ra,
            send_sem=a_sem.at[0],
            recv_sem=a_sem.at[1],
            device_id=peer,
            device_id_type=MESH,
        )

    def row_cols(r):
        return pl.ds(pl.multiple_of(r * rw, rw), rw)

    def b_copy(d):
        to = (my_row + d) % rows
        return pltpu.make_async_remote_copy(
            src_ref=sb.at[:, row_cols(to)],
            dst_ref=rb.at[d],
            send_sem=b_send.at[d],
            recv_sem=b_recv.at[d],
            device_id=(to, my_col),
            device_id_type=MESH,
        )

    def c_copy(r, origin):
        return pltpu.make_async_remote_copy(
            src_ref=rc.at[origin],
            dst_ref=rc.at[origin],
            send_sem=c_send.at[r],
            recv_sem=c_recv.at[r],
            device_id=chip_dev(r),
            device_id_type=MESH,
        )

    def d_copy(d, origin):
        part = fin.at[parity, :, row_cols(origin)]
        return pltpu.make_async_remote_copy(
            src_ref=part,
            dst_ref=part,
            send_sem=d_send.at[d],
            recv_sem=d_recv.at[d],
            device_id=row_dev(d),
            device_id_type=MESH,
        )

    def e_copy(part):
        return pltpu.make_async_remote_copy(
            src_ref=fin.at[part],
            dst_ref=fin.at[part],
            send_sem=e_sem.at[0],
            recv_sem=e_sem.at[1],
            device_id=peer,
            device_id_type=MESH,
        )

    def finish_group(t):
        c = group_cols(t)
        for which, (own, other) in enumerate(((kb, rk), (vb, rv))):
            grad_copy(t, which).wait_recv()
            own[:, c] = (own[:, c].astype(F32) + other[:, c].astype(F32)).astype(BF16)

    def sinks_b():
        a_copy().wait_recv()
        sb[...] = sg[parity] + ra[...]
        for d in range(1, rows):
            b_copy(d).start()

    def sinks_c():
        total = sb[:, row_cols(my_row)]
        for d in range(1, rows):
            b_copy(d).wait_recv()
            total = total + rb[d]
        rc[chip] = total
        for r in range(1, chips):
            c_copy(r, chip).start()

    def sinks_d():
        for r in range(1, chips):
            c_copy(r, flipped(chip, r)).wait_recv()
        total = rc[0]
        for r in range(1, chips):
            total = total + rc[r]
        fin[parity, :, row_cols(my_row)] = total.astype(BF16)
        for d in range(1, rows):
            d_copy(d, my_row).start()

    def sinks_e():
        for d in range(1, rows):
            d_copy(d, (my_row + rows - d) % rows).wait_recv()
        e_copy(parity).start()

    @pl.loop(0, GROUPS + 1)
    def _(i):
        @pl.when(i < GROUPS)
        def _():
            for which in range(2):
                kv_copy(i, which).wait_recv()

            @pl.loop(0, per_group // UNROLL)
            def _(j):
                attend(i * per_group + j * UNROLL)

            for which in range(2):
                grad_copy(i, which).start()

        @pl.when(i >= 1)
        def _():
            finish_group(i - 1)

        @pl.when(i < half)
        def _():
            forward(i)

        @pl.when(i >= half)
        def _():
            settle(i - half)

    a_copy().start()

    @pl.loop(0, WPARTS)
    def _(c):
        w_copy(c).wait()

    @pl.loop(0, CHUNKS)
    def _(c):
        share_in(c, 0).wait_recv()

    done = GROUPS + 1 - half

    @pl.loop(0, n_tiles)
    def _(n):
        whole_rows(0, n)

        @pl.when(n == 0)
        def _():
            sinks_b()

        @pl.when(n + done < half)
        def _():
            settle(n + done)

    @pl.loop(min(half, n_tiles + done), half)
    def _(j):
        settle(j)

    sinks_c()

    for level in range(2, levels):

        @pl.loop(0, half)
        def _(j):
            for r in range(1, chips):
                if bits(r) == level:
                    for tree in range(2):
                        pass_on(j, r, tree)

    for r in sorted(range(1, last), key=bits):

        @pl.loop(0, CHUNKS)
        def _(c):
            share_in(c, r).wait_recv()

        @pl.loop(0, n_tiles)
        def _(n):
            whole_rows(r, n)

    def take(j):
        for c in range(CHUNKS // PIECES):
            c = j * (CHUNKS // PIECES) + c
            hop_in(c, last).wait_recv()
            share(c, last).start()

    def mix(j, n, part):
        kcols = pl.ds(pl.multiple_of(j * pw, pw), pw)
        ncols = tile_cols(n)
        z = dot_nn(xg[rows_of(last), kcols], wv[kcols, ncols])
        if part == 0:
            acc[:, ncols] = z + bias[ncols]
        elif part == 1:
            acc[:, ncols] += z
        else:
            finish(acc[:, ncols] + z, last, ncols)

    take(0)
    take(1)
    for part, (lo, hi) in enumerate(((0, 1), (1, PIECES - 1), (PIECES - 1, PIECES))):

        @pl.loop(lo, hi)
        def _(j):
            for c in range(CHUNKS // PIECES):
                share_in(j * (CHUNKS // PIECES) + c, last).wait_recv()

            @pl.loop(0, n_tiles)
            def _(n):
                mix(j, n, part)

            @pl.when(j + 2 < PIECES)
            def _():
                take(j + 2)

            @pl.when(j == PIECES - 2)
            def _():
                sinks_d()

    sinks_e()

    @pl.loop(0, CHUNKS)
    def _(c):
        for r in range(chips):
            share(c, r).wait_send()
        for r in range(1, chips):
            hop_in(c, r).wait_send()

    @pl.loop(0, GROUPS)
    def _(t):
        for which in range(2):
            kv_copy(t, which).wait_send()
            grad_copy(t, which).wait_send()

    a_copy().wait_send()
    for d in range(1, rows):
        b_copy(d).wait_send()
        d_copy(d, my_row).wait_send()
    for r in range(1, chips):
        c_copy(r, chip).wait_send()
    e_copy(1 - parity).wait_recv()
    e_copy(parity).wait_send()


def store(ao, gq, gk, gv, fin, hid, ao_out, gq_out, gk_out, gv_out, gsk_out, gsv_out, hid_out, sem):
    copies = [
        pltpu.make_async_copy(src, dst, sem.at[s])
        for s, (src, dst) in enumerate(
            (
                (hid, hid_out),
                (ao, ao_out),
                (gq, gq_out),
                (gk, gk_out),
                (gv, gv_out),
                (fin.at[0], gsk_out),
                (fin.at[1], gsv_out),
            )
        )
    ]
    for copy in copies:
        copy.start()
    for copy in copies:
        copy.wait()


def local(
    rows,
    cols,
    query_grid,
    key_grid,
    value_grid,
    sink_keys,
    sink_values,
    grad_output,
    block_input,
    in_weight,
    in_bias,
):
    tile_rows, tile_cols, width = query_grid.shape
    tokens = tile_rows * tile_cols
    regs = sink_keys.shape[0]
    units = in_weight.shape[1]
    chips = cols // 2
    rw = width // rows

    def flat(a):
        return a.reshape(tokens, width)

    hbm = pl.BlockSpec(memory_space=pl.ANY)
    vmem = pl.BlockSpec(memory_space=pltpu.VMEM)
    shapes = ((tokens, width),) * 4 + (
        (2, regs, width),
        (tile_rows, cols * tile_cols, units),
    )
    dma = pltpu.SemaphoreType.DMA
    block = pltpu.VMEM((tokens, width), BF16)
    held = pl.pallas_call(
        functools.partial(kernel, rows, cols),
        out_shape=tuple(pltpu.VMEM(shape, BF16) for shape in shapes),
        in_specs=[hbm] * 6 + [vmem] * 3,
        out_specs=(vmem,) * 6,
        scratch_shapes=[block] * 4
        + [
            pltpu.VMEM((cols * tokens, width), BF16),
            pltpu.VMEM((width, units), BF16),
            pltpu.VMEM((2 * tokens, units), F32),
            pltpu.VMEM((2, regs, width), F32),
            pltpu.VMEM((regs, width), F32),
            pltpu.VMEM((regs, width), F32),
            pltpu.VMEM((rows, regs, rw), F32),
            pltpu.VMEM((chips, regs, rw), F32),
            pltpu.VMEM((16, width), BF16),
            pltpu.VMEM((16, width), BF16),
            dma((5,)),
            dma((WPARTS,)),
            dma((CHUNKS, chips)),
            dma((CHUNKS, chips)),
            dma((CHUNKS, chips)),
            dma((CHUNKS, chips)),
            dma((GROUPS, 2)),
            dma((GROUPS, 2)),
            dma((GROUPS, 2)),
            dma((GROUPS, 2)),
            dma((2,)),
            dma((rows,)),
            dma((rows,)),
            dma((chips,)),
            dma((chips,)),
            dma((rows,)),
            dma((rows,)),
            dma((2,)),
        ],
        compiler_params=pltpu.CompilerParams(
            collective_id=0, has_side_effects=True, vmem_limit_bytes=VMEM_LIMIT
        ),
        name="block",
    )(
        flat(query_grid),
        flat(key_grid),
        flat(value_grid),
        flat(grad_output),
        flat(block_input),
        in_weight,
        sink_keys,
        sink_values,
        in_bias,
    )
    grid = jax.ShapeDtypeStruct((tokens, width), BF16)
    sink = jax.ShapeDtypeStruct((regs, width), BF16)
    out = pl.pallas_call(
        store,
        out_shape=(grid,) * 4 + (sink,) * 2 + (jax.ShapeDtypeStruct(shapes[5], BF16),),
        in_specs=[vmem] * 6,
        out_specs=(hbm,) * 7,
        scratch_shapes=[dma((7,))],
        compiler_params=pltpu.CompilerParams(vmem_limit_bytes=1024 * 1024),
        name="store",
    )(*(pltpu.with_memory_space_constraint(a, pltpu.VMEM) for a in held))
    shaped = tuple(a.reshape(tile_rows, tile_cols, width) for a in out[:4])
    return shaped + out[4:]


def solution(mesh):
    placed = (
        P("row", "col", None),
        P("row", "col", None),
        P("row", "col", None),
        P(),
        P(),
        P("row", "col", None),
        P("row", "col", None),
        P(None, "col"),
        P("col"),
    )
    return jax.shard_map(
        functools.partial(local, mesh.shape["row"], mesh.shape["col"]),
        mesh=mesh,
        in_specs=placed,
        out_specs=(
            P("row", "col", None),
            P("row", "col", None),
            P("row", "col", None),
            P("row", "col", None),
            P(),
            P(),
            P("row", None, "col"),
        ),
        check_vma=False,
    )
```

```python
import functools
import math

import jax
import jax.numpy as jnp
from jax import lax
from jax.experimental import pallas as pl
from jax.experimental.pallas import tpu as pltpu
from jax.sharding import PartitionSpec as P

HEAD_DIM = 128
WIN = 16
MESH = pl.DeviceIdType.MESH
F32 = jnp.float32
BF16 = jnp.bfloat16
CHUNKS = 12
GROUPS = 8
UNROLL = 1
NT = 512
EARLY = 2
WPARTS = 6
VMEM_LIMIT = 50 * 1024 * 1024


def bits(r):
    return bin(r).count("1")


def parent(r, tree):
    if tree == 0:
        return r & ~(1 << (r.bit_length() - 1))
    return r & (r - 1)


def dot_nt(a, b):
    return lax.dot_general(a, b, (((1,), (1,)), ((), ())), preferred_element_type=F32)


def dot_nn(a, b):
    return lax.dot_general(a, b, (((1,), (0,)), ((), ())), preferred_element_type=F32)


def dot_tn(a, b):
    return lax.dot_general(a, b, (((0,), (0,)), ((), ())), preferred_element_type=F32)


def kernel(
    rows,
    cols,
    q_in,
    k_in,
    v_in,
    g_in,
    x_in,
    w_in,
    sk_in,
    sv_in,
    bias_in,
    gb,
    qb,
    kb,
    vb,
    fin,
    hid,
    pk,
    pv,
    rk,
    rv,
    xg,
    wv,
    acc,
    sg,
    ra,
    sb,
    rb,
    rc,
    sk,
    sv,
    bias,
    load_sem,
    w_sem,
    xs_sem,
    xr_sem,
    ps_sem,
    pr_sem,
    kvs_sem,
    kvr_sem,
    gs_sem,
    gr_sem,
    a_sem,
    b_send,
    b_recv,
    c_send,
    c_recv,
    d_send,
    d_recv,
    e_sem,
):
    tokens, width = q_in.shape
    units = w_in.shape[1]
    regs = fin.shape[1]
    chips = cols // 2
    levels = chips.bit_length() - 1
    last = chips - 1
    heads = width // HEAD_DIM
    per_group = heads // GROUPS
    kc = width // CHUNKS
    gw = width // GROUPS
    rw = width // rows
    wk = width // WPARTS
    pw = 2 * kc
    pair = 2 * tokens
    scale = 1.0 / math.sqrt(HEAD_DIM)
    nt = NT if units % NT == 0 else NT // 2
    n_tiles = units // nt

    my_row = lax.axis_index("row")
    my_col = lax.axis_index("col")
    parity = my_col % 2
    chip = my_col // 2
    peer = (my_row, my_col + 1 - 2 * parity)

    def flipped(value, mask):
        for b in range(levels):
            if mask >> b & 1:
                value = value + (1 << b) * (1 - 2 * ((value // (1 << b)) % 2))
        return value

    def chip_dev(r):
        return (my_row, flipped(chip, r) * 2 + parity)

    def row_dev(d):
        return ((my_row + d) % rows, my_col)

    def kids(r, tree):
        return [k for k in range(1, chips) if parent(k, tree) == r]

    def load(src, dst, s):
        return pltpu.make_async_copy(src, dst, load_sem.at[s])

    barrier = pltpu.get_barrier_semaphore()
    pl.semaphore_signal(barrier, inc=1, device_id=peer, device_id_type=MESH)
    for r in range(1, chips):
        pl.semaphore_signal(barrier, inc=1, device_id=chip_dev(r), device_id_type=MESH)
    for d in range(1, rows):
        pl.semaphore_signal(barrier, inc=1, device_id=row_dev(d), device_id_type=MESH)

    own_rows = pl.ds(pl.multiple_of(my_col * tokens, tokens), tokens)
    loads = (
        (q_in, qb),
        (k_in, kb),
        (v_in, vb),
        (g_in, gb),
        (sk_in, sk.at[:regs, :]),
        (sv_in, sv.at[:regs, :]),
        (bias_in, bias),
        (x_in, xg.at[own_rows, :]),
    )
    own = len(loads) - 1
    for pad in (sk, sv):
        pad[regs:, :] = jnp.zeros((pad.shape[0] - regs, width), BF16)

    for s in range(own):
        load(*loads[s], s).start()

    pl.semaphore_wait(barrier, 1 + chips - 1 + rows - 1)

    def group_cols(t):
        return pl.ds(pl.multiple_of(t * gw, gw), gw)

    def kv_copy(t, which):
        src, dst = ((k_in, pk), (v_in, pv))[which]
        c = group_cols(t)
        return pltpu.make_async_remote_copy(
            src_ref=src.at[:, c],
            dst_ref=dst.at[:, c],
            send_sem=kvs_sem.at[t, which],
            recv_sem=kvr_sem.at[t, which],
            device_id=peer,
            device_id_type=MESH,
        )

    def grad_copy(t, which):
        src, dst = ((pk, rk), (pv, rv))[which]
        c = group_cols(t)
        return pltpu.make_async_remote_copy(
            src_ref=src.at[:, c],
            dst_ref=dst.at[:, c],
            send_sem=gs_sem.at[t, which],
            recv_sem=gr_sem.at[t, which],
            device_id=peer,
            device_id_type=MESH,
        )

    def piece(c, r, core):
        origin = flipped(chip, r) * 2 + core
        return xg.at[
            pl.ds(pl.multiple_of(origin * tokens, tokens), tokens),
            pl.ds(pl.multiple_of(c * kc, kc), kc),
        ]

    def mine(c):
        return x_in.at[:, pl.ds(pl.multiple_of(c * kc, kc), kc)]

    def hop(c, r, up):
        block = piece(c, up, parity)
        return pltpu.make_async_remote_copy(
            src_ref=block if up else mine(c),
            dst_ref=block,
            send_sem=xs_sem.at[c, r],
            recv_sem=xr_sem.at[c, r],
            device_id=chip_dev(up ^ r),
            device_id_type=MESH,
        )

    def hop_in(c, r):
        block = piece(c, r, parity)
        return pltpu.make_async_remote_copy(
            src_ref=block,
            dst_ref=block,
            send_sem=xs_sem.at[c, r],
            recv_sem=xr_sem.at[c, r],
            device_id=chip_dev(1),
            device_id_type=MESH,
        )

    def share(c, r):
        block = piece(c, r, parity)
        return pltpu.make_async_remote_copy(
            src_ref=block if r else mine(c),
            dst_ref=block,
            send_sem=ps_sem.at[c, r],
            recv_sem=pr_sem.at[c, r],
            device_id=peer,
            device_id_type=MESH,
        )

    def share_in(c, r):
        block = piece(c, r, 1 - parity)
        return pltpu.make_async_remote_copy(
            src_ref=block,
            dst_ref=block,
            send_sem=ps_sem.at[c, r],
            recv_sem=pr_sem.at[c, r],
            device_id=peer,
            device_id_type=MESH,
        )

    def w_copy(c):
        part = pl.ds(pl.multiple_of(c * wk, wk), wk)
        return pltpu.make_async_copy(w_in.at[part, :], wv.at[part, :], w_sem.at[c])

    firsts = [r for r in range(1, chips) if bits(r) == 1]

    def pass_on(j, r, tree):
        c = 2 * j + tree
        hop_in(c, r).wait_recv()
        for kid in kids(r, tree):
            hop(c, kid, r).start()
        share(c, r).start()

    def forward(j):
        for r in firsts:
            for tree in range(2):
                if kids(r, tree):
                    pass_on(j, r, tree)

    def settle(j):
        for r in firsts:
            for tree in range(2):
                if not kids(r, tree):
                    pass_on(j, r, tree)

    half = CHUNKS // 2

    for which in range(2):
        kv_copy(0, which).start()
    for leaf in range(2):

        @pl.loop(0, half)
        def _(j):
            for r in firsts:
                for tree in range(2):
                    if bool(kids(r, tree)) != bool(leaf):
                        hop(2 * j + tree, r, 0).start()

    @pl.loop(1, GROUPS)
    def _(t):
        for which in range(2):
            kv_copy(t, which).start()

    @pl.loop(0, CHUNKS)
    def _(c):
        share(c, 0).start()

    load(*loads[own], own).start()

    @pl.loop(0, WPARTS)
    def _(c):
        w_copy(c).start()

    for s in range(own):
        load(*loads[s], s).wait()

    n_keys = pair + regs
    fill = sk.shape[0] - regs
    to_log2 = scale * math.log2(math.e)

    def diagonal(a):
        blank = jnp.zeros((tokens, HEAD_DIM), BF16)
        return jnp.concatenate(
            [
                jnp.concatenate([a[:, :HEAD_DIM], blank], axis=1),
                jnp.concatenate([blank, a[:, HEAD_DIM:]], axis=1),
            ],
            axis=0,
        )

    def padded(a):
        return jnp.concatenate([a, jnp.zeros((fill, a.shape[1]), F32)], axis=0).astype(BF16)

    def attend(first):
        at = [
            pl.ds(pl.multiple_of((first + 2 * j) * HEAD_DIM, 2 * HEAD_DIM), 2 * HEAD_DIM)
            for j in range(UNROLL)
        ]
        done = []
        for c in at:
            keys = jnp.concatenate([kb[:, c], pk[:, c], sk[:, c]], axis=0)
            values = jnp.concatenate([vb[:, c], pv[:, c], sv[:, c]], axis=0)
            qd = diagonal(qb[:, c])
            gd = diagonal(gb[:, c])
            s = dot_nt(keys, qd)[:n_keys] * to_log2
            dp = dot_nt(values, gd)[:n_keys]
            e = jnp.exp2(s - jnp.max(s, axis=0, keepdims=True))
            inv = 1.0 / jnp.sum(e, axis=0, keepdims=True)
            delta = jnp.sum(e * dp, axis=0, keepdims=True) * inv
            weight = padded(e * inv)
            ds = padded((e * (inv * scale)) * (dp - delta))
            dv = dot_nn(weight, gd)
            dk = dot_nn(ds, qd)
            o = []
            dq = []
            for h in range(2):
                at_h = slice(h * HEAD_DIM, (h + 1) * HEAD_DIM)
                o.append(dot_tn(weight[:, at_h], values[:, at_h]))
                dq.append(dot_tn(ds[:, at_h], keys[:, at_h]))
            done.append((o, dq, dk, dv))
        for c, (o, dq, dk, dv) in zip(at, done):
            gb[:, c] = jnp.concatenate(o, axis=1).astype(BF16)
            qb[:, c] = jnp.concatenate(dq, axis=1).astype(BF16)
            kb[:, c] = dk[:tokens].astype(BF16)
            pk[:, c] = dk[tokens:pair].astype(BF16)
            vb[:, c] = dv[:tokens].astype(BF16)
            pv[:, c] = dv[tokens:pair].astype(BF16)
            sg[0, :, c] = dk[pair:n_keys]
            sg[1, :, c] = dv[pair:n_keys]

    def rows_of(r):
        return pl.ds(pl.multiple_of(flipped(chip, r) * pair, pair), pair)

    def finish(z, r, ncols):
        y = 0.5 * z * (1.0 + lax.erf(z * math.sqrt(0.5)))
        y = y.astype(BF16)
        per = tokens // WIN
        first = flipped(chip, r) * (2 * per)
        for j in range(2):
            hid[:, pl.ds(pl.multiple_of(first + j * per, per), per), ncols] = y[
                j * tokens : (j + 1) * tokens
            ].reshape(WIN, per, nt)

    def tile_cols(n):
        return pl.ds(pl.multiple_of(n * nt, nt), nt)

    def whole_rows(r, n):
        ncols = tile_cols(n)
        z = dot_nn(xg[rows_of(r), :], wv[:, ncols]) + bias[ncols]
        finish(z, r, ncols)

    def a_copy():
        return pltpu.make_async_remote_copy(
            src_ref=sg.at[1 - parity],
            dst_ref=ra,
            send_sem=a_sem.at[0],
            recv_sem=a_sem.at[1],
            device_id=peer,
            device_id_type=MESH,
        )

    def row_cols(r):
        return pl.ds(pl.multiple_of(r * rw, rw), rw)

    def b_copy(d):
        to = (my_row + d) % rows
        return pltpu.make_async_remote_copy(
            src_ref=sb.at[:, row_cols(to)],
            dst_ref=rb.at[d],
            send_sem=b_send.at[d],
            recv_sem=b_recv.at[d],
            device_id=(to, my_col),
            device_id_type=MESH,
        )

    def c_copy(r, origin):
        return pltpu.make_async_remote_copy(
            src_ref=rc.at[origin],
            dst_ref=rc.at[origin],
            send_sem=c_send.at[r],
            recv_sem=c_recv.at[r],
            device_id=chip_dev(r),
            device_id_type=MESH,
        )

    def d_copy(d, origin):
        part = fin.at[parity, :, row_cols(origin)]
        return pltpu.make_async_remote_copy(
            src_ref=part,
            dst_ref=part,
            send_sem=d_send.at[d],
            recv_sem=d_recv.at[d],
            device_id=row_dev(d),
            device_id_type=MESH,
        )

    def e_copy(part):
        return pltpu.make_async_remote_copy(
            src_ref=fin.at[part],
            dst_ref=fin.at[part],
            send_sem=e_sem.at[0],
            recv_sem=e_sem.at[1],
            device_id=peer,
            device_id_type=MESH,
        )

    def finish_group(t):
        c = group_cols(t)
        for which, (own, other) in enumerate(((kb, rk), (vb, rv))):
            grad_copy(t, which).wait_recv()
            own[:, c] = (own[:, c].astype(F32) + other[:, c].astype(F32)).astype(BF16)

    def sinks_b():
        a_copy().wait_recv()
        sb[...] = sg[parity] + ra[...]
        for d in range(1, rows):
            b_copy(d).start()

    def sinks_c():
        total = sb[:, row_cols(my_row)]
        for d in range(1, rows):
            b_copy(d).wait_recv()
            total = total + rb[d]
        rc[chip] = total.astype(BF16)
        for r in range(1, chips):
            c_copy(r, chip).start()

    def sinks_d():
        for r in range(1, chips):
            c_copy(r, flipped(chip, r)).wait_recv()
        total = rc[0].astype(F32)
        for r in range(1, chips):
            total = total + rc[r].astype(F32)
        fin[parity, :, row_cols(my_row)] = total.astype(BF16)
        for d in range(1, rows):
            d_copy(d, my_row).start()

    def sinks_e():
        for d in range(1, rows):
            d_copy(d, (my_row + rows - d) % rows).wait_recv()
        e_copy(parity).start()

    @pl.loop(0, GROUPS + 1)
    def _(i):
        @pl.when(i < GROUPS)
        def _():
            for which in range(2):
                kv_copy(i, which).wait_recv()

            @pl.loop(0, per_group // (2 * UNROLL))
            def _(j):
                attend(i * per_group + j * 2 * UNROLL)

            for which in range(2):
                grad_copy(i, which).start()

        @pl.when(i >= 1)
        def _():
            finish_group(i - 1)

        for j in range(EARLY):

            @pl.when(i == GROUPS - 2 * (EARLY - j))
            def _():
                forward(j)

    a_copy().start()
    for n in range(n_tiles):
        ncols = tile_cols(n)
        acc[:, ncols] = jnp.broadcast_to(bias[ncols], (last * pair, nt))
    load(*loads[own], own).wait()

    @pl.loop(0, WPARTS)
    def _(c):
        w_copy(c).wait()

    @pl.loop(0, CHUNKS)
    def _(c):
        share_in(c, 0).wait_recv()

    @pl.loop(0, n_tiles)
    def _(n):
        whole_rows(0, n)

        @pl.when(n == 0)
        def _():
            sinks_b()

        @pl.when(n == n_tiles - 1)
        def _():
            sinks_c()

    @pl.loop(EARLY, half)
    def _(j):
        forward(j)

    def sum_rows(r):
        return slice((r - 1) * pair, r * pair)

    def mix(j, r):
        kcols = pl.ds(pl.multiple_of(j * pw, pw), pw)
        x = xg[rows_of(r), kcols]
        for n in range(n_tiles):
            ncols = tile_cols(n)
            acc[sum_rows(r), ncols] += dot_nn(x, wv[kcols, ncols])

    for level in range(1, levels + 1):
        here = [r for r in range(1, chips) if bits(r) == level]

        @pl.loop(0, half + 1)
        def _(j):
            @pl.when(j < half)
            def _():
                if level == 1:
                    settle(j)
                else:
                    for r in here:
                        for tree in range(2):
                            pass_on(j, r, tree)

            @pl.when(j >= 1)
            def _():
                for r in here:
                    for tree in range(2):
                        share_in(2 * (j - 1) + tree, r).wait_recv()
                    mix(j - 1, r)

            if level == levels:

                @pl.when(j == half - 3)
                def _():
                    sinks_d()

                @pl.when(j == half - 1)
                def _():
                    sinks_e()

        for r in here:

            @pl.loop(0, n_tiles)
            def _(n):
                ncols = tile_cols(n)
                finish(acc[sum_rows(r), ncols], r, ncols)

    @pl.loop(0, CHUNKS)
    def _(c):
        for r in range(chips):
            share(c, r).wait_send()
        for r in range(1, chips):
            hop_in(c, r).wait_send()

    @pl.loop(0, GROUPS)
    def _(t):
        for which in range(2):
            kv_copy(t, which).wait_send()
            grad_copy(t, which).wait_send()

    a_copy().wait_send()
    for d in range(1, rows):
        b_copy(d).wait_send()
        d_copy(d, my_row).wait_send()
    for r in range(1, chips):
        c_copy(r, chip).wait_send()
    e_copy(1 - parity).wait_recv()
    e_copy(parity).wait_send()


def store(ao, gq, gk, gv, fin, hid, ao_out, gq_out, gk_out, gv_out, gsk_out, gsv_out, hid_out, sem):
    copies = [
        pltpu.make_async_copy(src, dst, sem.at[s])
        for s, (src, dst) in enumerate(
            (
                (hid, hid_out),
                (ao, ao_out),
                (gq, gq_out),
                (gk, gk_out),
                (gv, gv_out),
                (fin.at[0], gsk_out),
                (fin.at[1], gsv_out),
            )
        )
    ]
    for copy in copies:
        copy.start()
    for copy in copies:
        copy.wait()


def local(
    rows,
    cols,
    query_grid,
    key_grid,
    value_grid,
    sink_keys,
    sink_values,
    grad_output,
    block_input,
    in_weight,
    in_bias,
):
    tile_rows, tile_cols, width = query_grid.shape
    tokens = tile_rows * tile_cols
    regs = sink_keys.shape[0]
    units = in_weight.shape[1]
    chips = cols // 2
    rw = width // rows

    def flat(a):
        return a.reshape(tokens, width)

    hbm = pl.BlockSpec(memory_space=pl.ANY)
    vmem = pl.BlockSpec(memory_space=pltpu.VMEM)
    shapes = ((tokens, width),) * 4 + (
        (2, regs, width),
        (tile_rows, cols * tile_cols, units),
    )
    dma = pltpu.SemaphoreType.DMA
    block = pltpu.VMEM((tokens, width), BF16)
    held = pl.pallas_call(
        functools.partial(kernel, rows, cols),
        out_shape=tuple(pltpu.VMEM(shape, BF16) for shape in shapes),
        in_specs=[hbm] * 9,
        out_specs=(vmem,) * 6,
        scratch_shapes=[block] * 4
        + [
            pltpu.VMEM((cols * tokens, width), BF16),
            pltpu.VMEM((width, units), BF16),
            pltpu.VMEM(((chips - 1) * 2 * tokens, units), F32),
            pltpu.VMEM((2, regs, width), F32),
            pltpu.VMEM((regs, width), F32),
            pltpu.VMEM((regs, width), F32),
            pltpu.VMEM((rows, regs, rw), F32),
            pltpu.VMEM((chips, regs, rw), BF16),
            pltpu.VMEM((16, width), BF16),
            pltpu.VMEM((16, width), BF16),
            pltpu.VMEM((units,), F32),
            dma((8,)),
            dma((WPARTS,)),
            dma((CHUNKS, chips)),
            dma((CHUNKS, chips)),
            dma((CHUNKS, chips)),
            dma((CHUNKS, chips)),
            dma((GROUPS, 2)),
            dma((GROUPS, 2)),
            dma((GROUPS, 2)),
            dma((GROUPS, 2)),
            dma((2,)),
            dma((rows,)),
            dma((rows,)),
            dma((chips,)),
            dma((chips,)),
            dma((rows,)),
            dma((rows,)),
            dma((2,)),
        ],
        compiler_params=pltpu.CompilerParams(
            collective_id=0, has_side_effects=True, vmem_limit_bytes=VMEM_LIMIT
        ),
        name="block",
    )(
        flat(query_grid),
        flat(key_grid),
        flat(value_grid),
        flat(grad_output),
        flat(block_input),
        in_weight,
        sink_keys,
        sink_values,
        in_bias,
    )
    grid = jax.ShapeDtypeStruct((tokens, width), BF16)
    sink = jax.ShapeDtypeStruct((regs, width), BF16)
    out = pl.pallas_call(
        store,
        out_shape=(grid,) * 4 + (sink,) * 2 + (jax.ShapeDtypeStruct(shapes[5], BF16),),
        in_specs=[vmem] * 6,
        out_specs=(hbm,) * 7,
        scratch_shapes=[dma((7,))],
        compiler_params=pltpu.CompilerParams(vmem_limit_bytes=1024 * 1024),
        name="store",
    )(*(pltpu.with_memory_space_constraint(a, pltpu.VMEM) for a in held))
    shaped = tuple(a.reshape(tile_rows, tile_cols, width) for a in out[:4])
    return shaped + out[4:]


def solution(mesh):
    placed = (
        P("row", "col", None),
        P("row", "col", None),
        P("row", "col", None),
        P(),
        P(),
        P("row", "col", None),
        P("row", "col", None),
        P(None, "col"),
        P("col"),
    )
    return jax.shard_map(
        functools.partial(local, mesh.shape["row"], mesh.shape["col"]),
        mesh=mesh,
        in_specs=placed,
        out_specs=(
            P("row", "col", None),
            P("row", "col", None),
            P("row", "col", None),
            P("row", "col", None),
            P(),
            P(),
            P("row", None, "col"),
        ),
        check_vma=False,
    )
```
